32 devices in a mesh: row: 4 (over y, x), col: 8 (over z, core).
Axes of the slice: x: 2, y: 2, z: 4, core: 2. Of those that a mesh axis runs over, the one named last changes fastest.
Arguments:
- basis_values: bfloat16 [8, 4, 4096, 256], P('col', 'row'), may hold values from -6 to 6
- weights: float32 [8, 4, 4096], P('col', 'row'), may hold values from 0.00390625 to 0.03125
- kernel: float32 [8, 4, 4096], P('col', 'row'), may hold values from -2 to -0.25
- live_points: int32 [8, 4], P('col', 'row'), may hold values from 1024 to 4096
- batch_tiles: int32 [8, 4, 2], P('col', 'row'), may hold values from 0 to 31, as said below
- density: bfloat16 [8, 4, 2, 2, 128, 128], P('col', 'row'), may hold values from -0.03125 to 0.03125
- tile_lists: int32 [8, 4, 2], P('col', 'row'), may hold values from 0 to 31, as said below
Outputs:
- hamiltonian: float32 [8, 4, 2, 2, 128, 128], P('col', 'row')
The draws below stay inside these ranges and needn't reach their ends.
Inputs may be any that keep to these rules, and one draw needn't show every extreme that they name: `batch_tiles`: tile t belongs to column t // 4. The first tile of the batch on column c belongs to column c, and each tile is the first tile of exactly one batch; the second tile differs from the first and belongs to column c - 1, c or c + 1, taken cyclically over 8 columns. `tile_lists`: each tile row of column c is held by exactly one device of column c, and its list starts with the row itself. The list of tile row t equals the list of the batch whose first tile is t.
All inputs are finite; a program needn't handle non-finite values.
Results may differ from the reference program's by a relative error of at most 0.0044.
Values may be sent and summed in bfloat16 or wider, within the bound.
No kernel may reach another device: no remote copies, remote signals or barrier semaphores. Data moves between devices by JAX's collectives and lax.ppermute only.
A program may use at most 64 MiB of HBM per device.

```python
import math
import jax
import jax.numpy as jnp
from jax import lax

TILE = 128
LIST = 2
POINTS = 4096
BASIS = 256
N_ROW = 4
N_COL = 8


def layout(key):
    owner_key = jax.random.fold_in(key, 101)
    home_key = jax.random.fold_in(key, 202)
    partner_key = jax.random.fold_in(key, 303)
    owner = jax.vmap(lambda sub_key: jax.random.permutation(sub_key, N_ROW))(jax.random.split(owner_key, N_COL)).astype(jnp.int32)
    home = jax.vmap(lambda sub_key: jax.random.permutation(sub_key, N_ROW))(jax.random.split(home_key, N_COL)).astype(jnp.int32)
    chosen = jax.random.randint(partner_key, (N_COL, N_ROW), 0, 3 * N_ROW - 1).astype(jnp.int32)
    within = jnp.arange(N_ROW, dtype=jnp.int32)[None, :]
    chosen = chosen + (chosen >= N_ROW + within).astype(jnp.int32)
    column = jnp.arange(N_COL, dtype=jnp.int32)[:, None]
    group = (column - 1 + chosen // N_ROW) % N_COL
    partner = group * N_ROW + chosen % N_ROW
    return (owner, home, partner)


def listing(held, partner):
    column = jnp.arange(N_COL, dtype=jnp.int32)[:, None]
    head = column * N_ROW + held
    tail = jnp.take_along_axis(partner, held, axis=1)
    return jnp.stack([head, tail], -1).astype(jnp.int32)


def draw_batch_tiles(key, part):
    owner, home, partner = layout(key)
    return listing(home, partner)


def draw_tile_lists(key, part):
    owner, home, partner = layout(key)
    return listing(owner, partner)


def place_ends(result, stream_key, smallest, high):
    extent = result.shape
    place = [jax.random.randint(jax.random.fold_in(stream_key, axis), (), 0, extent[axis]) for axis in range(len(extent))]
    result = result.at[tuple(place)].set(smallest)
    longest = extent.index(max(extent))
    place[longest] = (place[longest] + 1) % extent[longest]
    return result.at[tuple(place)].set(high)


def block_levels(own_key, shape, pieces, least, high):
    loudness = 1.0
    for position, blocks in pieces:
        draws = jax.random.uniform(jax.random.fold_in(jax.random.fold_in(own_key, 6), position), (blocks,), jnp.float32, least / len(pieces), high / len(pieces))
        loudness = loudness * jnp.repeat(jnp.exp(draws), shape[position] // blocks).reshape((-1,) + (1,) * (len(shape) - 1 - position))
    return loudness


def noise(rng, extent, deviation, limit, pieces=(), kind=jnp.bfloat16):
    result = jax.random.normal(rng, extent, jnp.float32) * deviation
    if len(pieces) > 0:
        result = block_levels(rng, extent, pieces, -0.22, 0.18) * result
    return jnp.clip(result, min=-limit, max=limit).astype(kind)


def setup_inputs(seed: int = 0) -> dict:
    keys = jax.random.split(jax.random.key(seed), 8)
    return {
        "basis_values": noise(keys[0], (N_COL, N_ROW, POINTS, BASIS), 1.0, 6.0, ((0, 8), (1, 4))),
        "weights": jnp.clip(jnp.exp(math.log(0.03125) - 2.0794415 * jax.random.uniform(keys[1], (N_COL, N_ROW, POINTS), jnp.float32) ** block_levels(keys[1], (N_COL, N_ROW, POINTS), ((0, 8), (1, 4)), -0.2, 0.2)), 0.00390625, 0.03125),
        "kernel": jnp.clip(-2.0 + 1.75 * jax.random.uniform(keys[2], (N_COL, N_ROW, POINTS), jnp.float32) ** block_levels(keys[2], (N_COL, N_ROW, POINTS), ((0, 8), (1, 4)), -0.2, 0.2), -2.0, -0.25),
        "live_points": place_ends(jax.random.randint(keys[3], (N_COL, N_ROW), POINTS // 4, POINTS + 1), jax.random.fold_in(keys[3], 1), POINTS // 4, POINTS).astype(jnp.int32),
        "batch_tiles": draw_batch_tiles(jax.random.fold_in(keys[7], 71), 0),
        "density": noise(keys[5], (N_COL, N_ROW, LIST, 2, TILE, TILE), (2 * TILE * TILE) ** -0.5, 0.03125, ((0, 8), (1, 4))),
        "tile_lists": draw_tile_lists(jax.random.fold_in(keys[7], 71), 0),
    }


def pair_ids(listed):
    head = listed[..., 0]
    tail = listed[..., 1]
    pair_rows = jnp.stack([head, head, tail, tail], -1)
    pair_cols = jnp.stack([head, tail, head, tail], -1)
    return pair_rows, pair_cols


def response(values, weight_row, kernel_row, live_count, tiles):
    points, basis = values.shape
    width = tiles.shape[-1]
    upper_half = jnp.concatenate([tiles[0], tiles[1]], 2)
    lower_half = jnp.concatenate([tiles[2], tiles[3]], 2)
    local = jnp.concatenate([upper_half, lower_half], 1)
    joined = jnp.concatenate([local[0], local[1]], 1)
    projected = jnp.dot(values, joined, preferred_element_type=jnp.float32)
    density_one = jnp.sum(projected[:, :basis] * values, axis=1)
    density_two = jnp.sum(projected[:, basis:] * values, axis=1)
    alive = (jnp.arange(points, dtype=jnp.int32) < live_count).astype(jnp.float32)
    factor = alive * weight_row * kernel_row
    scaled = jnp.concatenate([
        ((factor * density_one)[:, None] * values).astype(jnp.bfloat16),
        ((factor * density_two)[:, None] * values).astype(jnp.bfloat16)], 1)
    hamilton = lax.dot_general(values, scaled, (((0,), (0,)), ((), ())), preferred_element_type=jnp.float32)
    blocks = []
    for left_index in (0, 1):
        for right_index in (0, 1):
            per_pert = []
            for pert_index in (0, 1):
                start_col = pert_index * basis + right_index * width
                per_pert.append(hamilton[left_index * width:(left_index + 1) * width, start_col:start_col + width])
            blocks.append(jnp.stack(per_pert))
    return jnp.stack(blocks)


def reference(basis_values, weights, kernel, live_points, batch_tiles, density, tile_lists):
    list_len = tile_lists.shape[2]
    total = N_ROW * N_COL
    slots = total * list_len
    points = basis_values.shape[2]
    basis = basis_values.shape[3]
    flat_rows = jnp.broadcast_to(tile_lists[..., :1], tile_lists.shape).reshape(slots)
    flat_cols = tile_lists.reshape(slots)
    index_map = jnp.zeros((total * total,), jnp.int32).at[flat_rows * total + flat_cols].set(jnp.arange(slots, dtype=jnp.int32) + 1)
    tiles_all = density.reshape((slots,) + density.shape[3:])

    def one_batch(item):
        values, weight_row, kernel_row, live_count, listed = item
        pair_rows, pair_cols = pair_ids(listed)
        slot_ids = index_map[pair_rows * total + pair_cols] - 1
        found = tiles_all[jnp.maximum(slot_ids, 0)]
        tiles = jnp.where((slot_ids >= 0)[:, None, None, None], found, jnp.zeros((), tiles_all.dtype))
        return response(values, weight_row, kernel_row, live_count, tiles), slot_ids

    partials, slot_ids = lax.map(one_batch, (
        basis_values.reshape(total, points, basis),
        weights.reshape(total, points),
        kernel.reshape(total, points),
        live_points.reshape(total),
        batch_tiles.reshape(total, list_len)))
    segment_ids = jnp.where(slot_ids >= 0, slot_ids, slots).reshape(total * 4).astype(jnp.int32)
    summed = jax.ops.segment_sum(partials.reshape((total * 4,) + partials.shape[2:]), segment_ids, num_segments=slots + 1)
    return summed[:slots].reshape(density.shape)
```

```python
import functools

import jax
import jax.numpy as jnp
from jax import lax
from jax.experimental import pallas as pl
from jax.experimental.pallas import tpu as pltpu
from jax.sharding import PartitionSpec as P

DIGIT = 256
ID_ROWS = 16


def row_route(count, step):
    if count & (count - 1) == 0:
        return [(i, i ^ step) for i in range(count)]
    return [(i, (i + step) % count) for i in range(count)]


def from_peer(block, step):
    return lax.ppermute(block, "row", row_route(lax.axis_size("row"), step))


def to_peer(block, step):
    route = row_route(lax.axis_size("row"), step)
    return lax.ppermute(block, "row", [(target, source) for source, target in route])


def passed_along(block, distance):
    count = lax.axis_size("col")
    return lax.ppermute(block, "col", [((i - distance) % count, i) for i in range(count)])


VMEM = pl.BlockSpec(memory_space=pltpu.VMEM)
SMEM = pl.BlockSpec(memory_space=pltpu.SMEM)


def pack_body(lists, batch, tiles, message, wanted):
    size = tiles.shape[0]
    message[:size, :] = tiles[...]
    row = lax.broadcasted_iota(jnp.int32, (ID_ROWS, tiles.shape[1]), 0)
    digits = jnp.zeros(row.shape, jnp.int32)
    for place in (0, 1):
        tile = lists[place]
        digits = jnp.where(row == 2 * place, tile % DIGIT, digits)
        digits = jnp.where(row == 2 * place + 1, tile // DIGIT, digits)
    message[size:, :] = digits.astype(jnp.float32).astype(message.dtype)
    slot = lax.broadcasted_iota(jnp.int32, wanted.shape, 0)
    wanted[...] = jnp.where(slot == 0, batch[0], batch[1])


def values_body(live, values, weights, kernel, turned, factor):
    points = values.shape[0]
    step = 512
    for start in range(0, points, step):
        turned[:, start : start + step] = values[start : start + step, :].T
    point = lax.broadcasted_iota(jnp.int32, weights.shape, 1)
    factor[...] = jnp.where(point < live[0, 0], weights[...] * kernel[...], 0.0)


def row_ids(message, size):
    digits = message[size:, :].astype(jnp.float32).astype(jnp.int32)
    head = digits[0:1] + DIGIT * digits[1:2]
    tail = digits[2:3] + DIGIT * digits[3:4]
    return head, tail


def route_body(*refs, rows):
    messages = refs[:rows]
    own, lower, upper = refs[rows : rows + 3]
    first, second, for_lower, for_upper = refs[rows + 3 :]
    width = messages[0].shape[1]
    size = 4 * width
    ids = [row_ids(m, size) for m in messages]

    def pick(mask_of, offset):
        total = jnp.zeros((width, width), jnp.bfloat16)
        for m, (head, tail) in zip(messages, ids):
            mask = mask_of(head, tail)
            tile = m[offset : offset + width, :]
            total = jnp.where(mask, tile, total)
        return total

    for pert in (0, 1):
        diag = pert * width
        cross = (2 + pert) * width
        s0, s1 = own[0:1, :], own[1:2, :]
        rows_at = slice(pert * width, (pert + 1) * width)
        first[rows_at, :width] = pick(lambda h, t: h == s0, diag)
        first[rows_at, width:] = pick(lambda h, t: (h == s0) & (t == s1), cross)
        for ref, want in ((second, own), (for_lower, lower), (for_upper, upper)):
            w0, w1 = want[0:1, :], want[1:2, :]
            ref[rows_at, :width] = pick(lambda h, t: (h == w1) & (t == w0), cross)
            ref[rows_at, width:] = pick(lambda h, t: h == w1, diag)


def quadratic(matrix, turned, chunk, rows):
    width = matrix.shape[0] // 2
    product = jnp.dot(matrix, turned[:, chunk], preferred_element_type=jnp.float32)
    side = turned[rows, chunk].astype(jnp.float32)
    return [
        jnp.sum(product[p * width : (p + 1) * width] * side, axis=0, keepdims=True) for p in (0, 1)
    ]


STEP = 512


def begin_body(first, turned, early):
    width = first.shape[0] // 2
    matrix = first[...]
    for start in range(0, turned.shape[1], STEP):
        chunk = slice(start, start + STEP)
        sums = quadratic(matrix, turned, chunk, slice(0, width))
        for p in (0, 1):
            early[p : p + 1, chunk] = sums[p]


def main_body(second, lower, upper, turned, values, early, factor, part, message, scaled):
    width = second.shape[0] // 2
    matrix = second[...] + lower[...] + upper[...]
    total = jnp.zeros(part.shape, jnp.float32)
    for start in range(0, turned.shape[1], STEP):
        chunk = slice(start, start + STEP)
        sums = quadratic(matrix, turned, chunk, slice(width, 2 * width))
        side = turned[:, chunk].astype(jnp.float32)
        lhs = []
        for p in (0, 1):
            potential = factor[:, chunk] * (early[p : p + 1, chunk] + sums[p])
            block = (potential * side).astype(jnp.bfloat16)
            scaled[p * width : (p + 1) * width, chunk] = block[:width]
            lhs.append(block[width:])
        total += jnp.dot(
            jnp.concatenate(lhs, 0), values[chunk, :], preferred_element_type=jnp.float32
        )
    part[...] = total
    message[...] = total.astype(jnp.bfloat16)


def rest_body(scaled, values, part):
    part[...] = jnp.dot(scaled[...], values[...], preferred_element_type=jnp.float32)


def collect_body(*refs, rows):
    messages = refs[:rows]
    own, lower, upper, first, second, from_lower, from_upper = refs[rows : rows + 7]
    outs = refs[rows + 7 :]
    width = messages[0].shape[1]
    size = 4 * width
    w = [(ref[0:1, :], ref[1:2, :]) for ref in (own, lower, upper)]
    for message, out in zip(messages, outs):
        head, tail = row_ids(message, size)
        is_first = head == w[0][0]
        for p in (0, 1):
            at = slice(p * width, (p + 1) * width)
            diag = jnp.where(is_first, first[at, :width], 0.0)
            cross = jnp.where(is_first & (tail == w[0][1]), first[at, width:], 0.0)
            for (s0, s1), ref in zip(w, (second, from_lower, from_upper)):
                block = ref[at, :].astype(jnp.float32)
                diag += jnp.where(head == s1, block[:, width:], 0.0)
                cross += jnp.where((head == s1) & (tail == s0), block[:, :width], 0.0)
            out[p * width : (p + 1) * width, :] = diag.astype(out.dtype)
            out[(2 + p) * width : (3 + p) * width, :] = cross.astype(out.dtype)


def sum_body(*refs):
    total = refs[0][...]
    for ref in refs[1:-1]:
        total += ref[...].astype(jnp.float32)
    refs[-1][...] = total


def on_device(basis_values, weights, kernel, live_points, batch_tiles, density, tile_lists):
    rows = lax.axis_size("row")
    width = density.shape[-1]
    points, basis = basis_values.shape[2:]
    f32, bf16 = jnp.float32, jnp.bfloat16
    shape = jax.ShapeDtypeStruct
    vmem = pltpu.VMEM
    size = 4 * width
    tiles = density.reshape(size, width)
    values = basis_values.reshape(points, basis)
    flops = 2 * points * basis * basis

    message, wanted = pl.pallas_call(
        pack_body,
        in_specs=[SMEM, SMEM, VMEM],
        out_specs=[VMEM, VMEM],
        out_shape=[shape((size + ID_ROWS, width), bf16), shape((8, width), jnp.int32)],
        name="pack",
    )(tile_lists.reshape(-1), batch_tiles.reshape(-1), tiles)
    messages = [message] + [from_peer(message, step) for step in range(1, rows)]
    want_lower = passed_along(wanted, 1)
    want_upper = passed_along(wanted, -1)
    wants = [wanted, want_lower, want_upper]

    turned, factor = pl.pallas_call(
        values_body,
        in_specs=[SMEM, VMEM, VMEM, VMEM],
        out_specs=[VMEM, VMEM],
        out_shape=[shape((basis, points), bf16), shape((1, points), f32)],
        name="turn",
        cost_estimate=pl.CostEstimate(flops=flops, bytes_accessed=0, transcendentals=0),
    )(live_points, values, weights.reshape(1, points), kernel.reshape(1, points))

    square = shape((2 * width, basis), bf16)
    first, second, for_lower, for_upper = pl.pallas_call(
        functools.partial(route_body, rows=rows),
        out_shape=[square] * 4,
        name="route",
    )(*messages, *wants)
    from_upper = passed_along(for_lower, -1)
    from_lower = passed_along(for_upper, 1)

    early = pl.pallas_call(
        begin_body,
        out_shape=shape((2, points), f32),
        name="begin",
        cost_estimate=pl.CostEstimate(flops=flops, bytes_accessed=0, transcendentals=0),
    )(first, turned)

    part_second, send, scaled = pl.pallas_call(
        main_body,
        out_shape=[
            shape((2 * width, basis), f32),
            square,
            shape((2 * width, points), bf16),
        ],
        name="main",
        cost_estimate=pl.CostEstimate(flops=2 * flops, bytes_accessed=0, transcendentals=0),
    )(second, from_lower, from_upper, turned, values, early, factor)
    sums_lower = passed_along(send, 1)
    sums_upper = passed_along(send, -1)

    part_first = pl.pallas_call(
        rest_body,
        out_shape=shape((2 * width, basis), f32),
        name="rest",
        cost_estimate=pl.CostEstimate(flops=flops, bytes_accessed=0, transcendentals=0),
    )(scaled, values)

    outs = pl.pallas_call(
        functools.partial(collect_body, rows=rows),
        out_shape=[shape((size, width), f32)] + [shape((size, width), bf16)] * (rows - 1),
        name="collect",
    )(*messages, *wants, part_first, part_second, sums_lower, sums_upper)
    received = [to_peer(outs[step], step) for step in range(1, rows)]
    owned = pl.pallas_call(sum_body, out_shape=shape((size, width), f32), name="add")(
        outs[0], *received
    )
    return owned.reshape(density.shape)


def solution(mesh):
    placed = (
        P("col", "row", None, None),
        P("col", "row", None),
        P("col", "row", None),
        P("col", "row"),
        P("col", "row", None),
        P("col", "row", None, None, None, None),
        P("col", "row", None),
    )
    return jax.shard_map(
        on_device,
        mesh=mesh,
        in_specs=placed,
        out_specs=P("col", "row", None, None, None, None),
        check_vma=False,
    )
```

```python
import functools

import jax
import jax.numpy as jnp
from jax import lax
from jax.experimental import pallas as pl
from jax.experimental.pallas import tpu as pltpu
from jax.sharding import PartitionSpec as P

DIGIT = 256
ID_ROWS = 16
LIMIT = 16 * 1024 * 1024


def row_route(count, step):
    if count & (count - 1) == 0:
        return [(i, i ^ step) for i in range(count)]
    return [(i, (i + step) % count) for i in range(count)]


def from_peer(block, step):
    return lax.ppermute(block, "row", row_route(lax.axis_size("row"), step))


def to_peer(block, step):
    route = row_route(lax.axis_size("row"), step)
    return lax.ppermute(block, "row", [(target, source) for source, target in route])


def col_routes(count):
    if count % 2 == 0:
        mate = [(i, i ^ 1) for i in range(count)]
        link = [(i, (i + 1 if i % 2 else i - 1) % count) for i in range(count)]
        return link, mate
    return ([(i, (i + step) % count) for i in range(count)] for step in (1, -1))


def to_sides(blocks):
    routes = col_routes(lax.axis_size("col"))
    return [lax.ppermute(block, "col", route) for block, route in zip(blocks, routes)]


def back_to_sides(blocks):
    routes = col_routes(lax.axis_size("col"))
    return [
        lax.ppermute(block, "col", [(target, source) for source, target in route])
        for block, route in zip(blocks, routes)
    ]


def run(name, body, outs, scalars, arrays, flops=0):
    return pl.pallas_call(
        body,
        in_specs=[pl.BlockSpec(memory_space=pltpu.SMEM)] * len(scalars)
        + [pl.BlockSpec(memory_space=pltpu.VMEM)] * len(arrays),
        out_shape=outs,
        name=name,
        cost_estimate=pl.CostEstimate(flops=flops, bytes_accessed=0, transcendentals=0),
        compiler_params=pltpu.CompilerParams(vmem_limit_bytes=LIMIT),
    )(*scalars, *(pltpu.with_memory_space_constraint(x, pltpu.VMEM) for x in arrays))


def in_hbm(x):
    return pltpu.with_memory_space_constraint(x, pltpu.HBM)


def pack_body(lists, batch, tiles, message, wanted, arrived):
    size = tiles.shape[0]
    copy = pltpu.make_async_copy(tiles, message.at[:size, :], arrived)
    copy.start()
    row = lax.broadcasted_iota(jnp.int32, (ID_ROWS, tiles.shape[1]), 0)
    digits = jnp.zeros(row.shape, jnp.int32)
    for place in (0, 1):
        tile = lists[place]
        digits = jnp.where(row == 2 * place, tile % DIGIT, digits)
        digits = jnp.where(row == 2 * place + 1, tile // DIGIT, digits)
    message[size:, :] = digits.astype(jnp.float32).astype(message.dtype)
    slot = lax.broadcasted_iota(jnp.int32, wanted.shape, 0)
    wanted[...] = jnp.where(slot == 0, batch[0], batch[1])
    copy.wait()


def values_body(live, after, values, weights, kernel, turned, kept, factor, other, arrived):
    points = values.shape[0]
    step = 512
    chunks = [slice(start, start + step) for start in range(0, points, step)]
    copies = [
        pltpu.make_async_copy(values.at[chunk, :], kept.at[chunk, :], arrived.at[i])
        for i, chunk in enumerate(chunks)
    ]
    side = [
        pltpu.make_async_copy(weights, factor, arrived.at[len(chunks)]),
        pltpu.make_async_copy(kernel, other, arrived.at[len(chunks) + 1]),
    ]
    for copy in copies + side:
        copy.start()
    for chunk, copy in zip(chunks, copies):
        copy.wait()
        turned[:, chunk] = kept[chunk, :].T
    for copy in side:
        copy.wait()
    point = lax.broadcasted_iota(jnp.int32, factor.shape, 1)
    factor[...] = jnp.where(point < live[0], factor[...] * other[...], 0.0)


def row_ids(message, size):
    digits = message[size:, :].astype(jnp.float32).astype(jnp.int32)
    head = digits[0:1] + DIGIT * digits[1:2]
    tail = digits[2:3] + DIGIT * digits[3:4]
    return head, tail


def route_body(*refs, rows):
    messages = refs[:rows]
    own, lower, upper = refs[rows : rows + 3]
    first, second, for_lower, for_upper = refs[rows + 4 :]
    width = messages[0].shape[1]
    size = 4 * width
    ids = [row_ids(m, size) for m in messages]

    def pick(mask_of, offset):
        total = jnp.zeros((width, width), jnp.bfloat16)
        for m, (head, tail) in zip(messages, ids):
            mask = mask_of(head, tail)
            tile = m[offset : offset + width, :]
            total = jnp.where(mask, tile, total)
        return total

    for pert in (0, 1):
        diag = pert * width
        cross = (2 + pert) * width
        s0, s1 = own[0:1, :], own[1:2, :]
        rows_at = slice(pert * width, (pert + 1) * width)
        first[rows_at, :width] = pick(lambda h, t: h == s0, diag)
        first[rows_at, width:] = pick(lambda h, t: (h == s0) & (t == s1), cross)
        for ref, want in ((second, own), (for_lower, lower), (for_upper, upper)):
            w0, w1 = want[0:1, :], want[1:2, :]
            ref[rows_at, :width] = pick(lambda h, t: (h == w1) & (t == w0), cross)
            ref[rows_at, width:] = pick(lambda h, t: h == w1, diag)


def quadratic(matrix, turned, chunk, rows):
    width = matrix.shape[0] // 2
    product = jnp.dot(matrix, turned[:, chunk], preferred_element_type=jnp.float32)
    side = turned[rows, chunk].astype(jnp.float32)
    return [
        jnp.sum(product[p * width : (p + 1) * width] * side, axis=0, keepdims=True) for p in (0, 1)
    ]


STEP = 512


def begin_body(first, turned, early):
    width = first.shape[0] // 2
    matrix = first[...]
    for start in range(0, turned.shape[1], STEP):
        chunk = slice(start, start + STEP)
        sums = quadratic(matrix, turned, chunk, slice(0, width))
        for p in (0, 1):
            early[p : p + 1, chunk] = sums[p]


def main_body(second, lower, upper, turned, values, early, factor, part, message, scaled):
    width = second.shape[0] // 2
    matrix = second[...] + lower[...] + upper[...]
    total = jnp.zeros(part.shape, jnp.float32)
    for start in range(0, turned.shape[1], STEP):
        chunk = slice(start, start + STEP)
        sums = quadratic(matrix, turned, chunk, slice(width, 2 * width))
        side = turned[:, chunk].astype(jnp.float32)
        lhs = []
        for p in (0, 1):
            potential = factor[:, chunk] * (early[p : p + 1, chunk] + sums[p])
            block = (potential * side).astype(jnp.bfloat16)
            scaled[p * width : (p + 1) * width, chunk] = block[:width]
            lhs.append(block[width:])
        total += jnp.dot(
            jnp.concatenate(lhs, 0), values[chunk, :], preferred_element_type=jnp.float32
        )
    part[...] = total
    message[...] = total.astype(jnp.bfloat16)


def rest_body(scaled, values, part):
    part[...] = jnp.dot(scaled[...], values[...], preferred_element_type=jnp.float32)


def collect_body(*refs, rows):
    messages = refs[:rows]
    own, lower, upper, first, second, from_lower, from_upper = refs[rows : rows + 7]
    outs = refs[rows + 7 :]
    width = messages[0].shape[1]
    size = 4 * width
    w = [(ref[0:1, :], ref[1:2, :]) for ref in (own, lower, upper)]
    for message, out in zip(messages, outs):
        head, tail = row_ids(message, size)
        is_first = head == w[0][0]
        for p in (0, 1):
            at = slice(p * width, (p + 1) * width)
            diag = jnp.where(is_first, first[at, :width], 0.0)
            cross = jnp.where(is_first & (tail == w[0][1]), first[at, width:], 0.0)
            for (s0, s1), ref in zip(w, (second, from_lower, from_upper)):
                block = ref[at, :].astype(jnp.float32)
                diag += jnp.where(head == s1, block[:, width:], 0.0)
                cross += jnp.where((head == s1) & (tail == s0), block[:, :width], 0.0)
            out[p * width : (p + 1) * width, :] = diag.astype(out.dtype)
            out[(2 + p) * width : (3 + p) * width, :] = cross.astype(out.dtype)


def sum_body(*refs):
    total = refs[0][...]
    for ref in refs[1:-1]:
        total += ref[...].astype(jnp.float32)
    refs[-1][...] = total


def on_device(basis_values, weights, kernel, live_points, batch_tiles, density, tile_lists):
    rows = lax.axis_size("row")
    width = density.shape[-1]
    points, basis = basis_values.shape[2:]
    f32, bf16 = jnp.float32, jnp.bfloat16
    size = 4 * width
    values = basis_values.reshape(points, basis)
    flops = 2 * points * basis * basis

    message, wanted = pl.pallas_call(
        pack_body,
        in_specs=[
            pl.BlockSpec(memory_space=pltpu.SMEM),
            pl.BlockSpec(memory_space=pltpu.SMEM),
            pl.BlockSpec(memory_space=pltpu.HBM),
        ],
        out_shape=[pltpu.VMEM((size + ID_ROWS, width), bf16), pltpu.VMEM((8, width), jnp.int32)],
        scratch_shapes=[pltpu.SemaphoreType.DMA],
        name="pack",
        compiler_params=pltpu.CompilerParams(vmem_limit_bytes=LIMIT),
    )(
        in_hbm(tile_lists.reshape(-1)),
        in_hbm(batch_tiles.reshape(-1)),
        in_hbm(density.reshape(size, width)),
    )
    messages = [message] + [from_peer(message, step) for step in range(1, rows)]
    wants = [wanted] + to_sides([wanted, wanted])

    hbm = pl.BlockSpec(memory_space=pltpu.HBM)
    turned, kept, factor = pl.pallas_call(
        values_body,
        in_specs=[
            pl.BlockSpec(memory_space=pltpu.SMEM),
            pl.BlockSpec(memory_space=pltpu.VMEM),
            hbm,
            hbm,
            hbm,
        ],
        out_shape=[
            pltpu.VMEM((basis, points), bf16),
            pltpu.VMEM((points, basis), bf16),
            pltpu.VMEM((1, points), f32),
        ],
        scratch_shapes=[
            pltpu.VMEM((1, points), f32),
            pltpu.SemaphoreType.DMA((points // 512 + 2,)),
        ],
        name="turn",
        cost_estimate=pl.CostEstimate(flops=flops, bytes_accessed=0, transcendentals=0),
        compiler_params=pltpu.CompilerParams(vmem_limit_bytes=LIMIT),
    )(
        live_points.reshape(-1),
        pltpu.with_memory_space_constraint(wanted, pltpu.VMEM),
        in_hbm(values),
        in_hbm(weights.reshape(1, points)),
        in_hbm(kernel.reshape(1, points)),
    )

    square = pltpu.VMEM((2 * width, basis), bf16)
    first, second, *answers = run(
        "route",
        functools.partial(route_body, rows=rows),
        [square] * 4,
        [],
        messages + wants + [factor],
    )
    answers = back_to_sides(answers)

    early = run(
        "begin", begin_body, pltpu.VMEM((2, points), f32), [], [first, turned], flops
    )

    part_second, send, scaled = run(
        "main",
        main_body,
        [
            pltpu.VMEM((2 * width, basis), f32),
            square,
            pltpu.VMEM((2 * width, points), bf16),
        ],
        [],
        [second, *answers, turned, kept, early, factor],
        2 * flops,
    )
    sums = to_sides([send, send])

    part_first = run(
        "rest",
        rest_body,
        pltpu.VMEM((2 * width, basis), f32),
        [],
        [scaled, kept],
        flops,
    )

    outs = run(
        "collect",
        functools.partial(collect_body, rows=rows),
        [pltpu.VMEM((size, width), f32)] + [pltpu.VMEM((size, width), bf16)] * (rows - 1),
        [],
        messages + wants + [part_first, part_second] + sums,
    )
    received = [to_peer(outs[step], step) for step in range(1, rows)]
    owned = run(
        "add", sum_body, jax.ShapeDtypeStruct((size, width), f32), [], [outs[0]] + received
    )
    return owned.reshape(density.shape)


def solution(mesh):
    placed = (
        P("col", "row", None, None),
        P("col", "row", None),
        P("col", "row", None),
        P("col", "row"),
        P("col", "row", None),
        P("col", "row", None, None, None, None),
        P("col", "row", None),
    )
    return jax.shard_map(
        on_device,
        mesh=mesh,
        in_specs=placed,
        out_specs=P("col", "row", None, None, None, None),
        check_vma=False,
    )
```
